16 devices in a mesh: ep: 16 (over z, y, x, core).
Axes of the slice: x: 2, y: 2, z: 2, core: 2. Of those that a mesh axis runs over, the one named last changes fastest.
Arguments:
- tokens: bfloat16 [8192, 2048], P('ep')
- expert_idx: int32 [8192], P('ep')
- w_router: bfloat16 [2048, 64], replicated
- w_in: bfloat16 [64, 2048, 1408], P('ep')
- w_out: bfloat16 [64, 1408, 2048], P('ep')
- loss_probe: bfloat16 [8192, 2048], P('ep')
Outputs:
- output 1: float32 [], replicated
- output 2: bfloat16 [8192, 2048], P('ep')
- output 3: bfloat16 [64, 2048, 1408], P('ep')
- output 4: bfloat16 [64, 1408, 2048], P('ep')
- output 5: float32 [2048, 64], replicated
All inputs are finite; a program needn't handle non-finite values.
Results may differ from the reference program's by a relative error of at most 0.00525.
Values are sent between devices in bfloat16 or wider.
A program may use at most 1 GiB of HBM per device.

```python
import jax
import jax.numpy as jnp
from jax import lax

GROUPS = 16
TOKENS_DEV = 512
HIDDEN = 2048
FFN_DIM = 1408
EXPERTS = 64
ALL_TOKENS = GROUPS * TOKENS_DEV
CAPACITY = (5 * ALL_TOKENS + 4 * EXPERTS - 1) // (4 * EXPERTS)
AUX_WEIGHT = 0.01
ROUTE_BOOST = 4.0


def draw_routing(base_key):
    half_experts = EXPERTS // 2
    per_pair = TOKENS_DEV // EXPERTS
    perm_key, extra_key, order_key = jax.random.split(base_key, 3)
    expert_perm = jax.random.permutation(perm_key, EXPERTS).astype(jnp.int32)
    hot_extra = jax.random.randint(extra_key, (GROUPS, half_experts), per_pair // 2, per_pair + 1)
    hot_extra = hot_extra.at[0, 0].set(per_pair)
    hot_rows = per_pair + hot_extra
    lane_ids = jnp.arange(2 * per_pair)
    is_hot = lane_ids[None, None, :] < hot_rows[:, :, None]
    labels = jnp.where(is_hot, expert_perm[:half_experts][None, :, None], expert_perm[half_experts:][None, :, None])
    labels = labels.reshape(GROUPS, TOKENS_DEV)
    order_keys = jax.random.split(order_key, GROUPS)
    orders = jax.vmap(lambda sub_key: jax.random.permutation(sub_key, TOKENS_DEV))(order_keys)
    return jnp.take_along_axis(labels, orders, axis=1).reshape(ALL_TOKENS).astype(jnp.int32)


def setup_inputs(seed: int = 0) -> dict:
    key_list = jax.random.split(jax.random.key(seed), 6)
    expert_idx = draw_routing(key_list[0])
    router_f = jax.random.normal(key_list[1], (HIDDEN, EXPERTS), jnp.float32) * HIDDEN ** -0.5
    tokens_f = jax.random.normal(key_list[2], (ALL_TOKENS, HIDDEN), jnp.float32) + ROUTE_BOOST * router_f.T[expert_idx]
    w_in = jax.random.normal(key_list[3], (EXPERTS, HIDDEN, FFN_DIM), jnp.float32) * HIDDEN ** -0.5
    w_out = jax.random.normal(key_list[4], (EXPERTS, FFN_DIM, HIDDEN), jnp.float32) * FFN_DIM ** -0.5
    loss_probe = jax.random.normal(key_list[5], (ALL_TOKENS, HIDDEN), jnp.float32)
    return {'tokens': tokens_f.astype(jnp.bfloat16), 'expert_idx': expert_idx, 'w_router': router_f.astype(jnp.bfloat16), 'w_in': w_in.astype(jnp.bfloat16), 'w_out': w_out.astype(jnp.bfloat16), 'loss_probe': loss_probe.astype(jnp.bfloat16)}


def expert_pass(operands):
    x_buf, g_buf, w_first, w_second = operands
    pre_act = jnp.dot(x_buf, w_first, preferred_element_type=jnp.float32)
    hidden = jnp.maximum(pre_act, 0.0).astype(jnp.bfloat16)
    z_buf = jnp.dot(hidden, w_second, preferred_element_type=jnp.float32).astype(jnp.bfloat16)
    grad_second = jnp.dot(hidden.T, g_buf, preferred_element_type=jnp.float32).astype(jnp.bfloat16)
    grad_hidden = jnp.dot(g_buf, w_second.T, preferred_element_type=jnp.float32)
    grad_pre = jnp.where(hidden > 0, grad_hidden, 0.0).astype(jnp.bfloat16)
    grad_first = jnp.dot(x_buf.T, grad_pre, preferred_element_type=jnp.float32).astype(jnp.bfloat16)
    u_buf = jnp.dot(grad_pre, w_first.T, preferred_element_type=jnp.float32).astype(jnp.bfloat16)
    return z_buf, u_buf, grad_first, grad_second


def reference(tokens, expert_idx, w_router, w_in, w_out, loss_probe):
    grad_scale = 1.0 / (ALL_TOKENS * HIDDEN)
    buffer_rows = EXPERTS * CAPACITY
    expert_ids = jnp.arange(EXPERTS, dtype=jnp.int32)
    onehot = (expert_idx[:, None] == expert_ids[None, :]).astype(jnp.int32)
    before = jnp.cumsum(onehot, axis=0) - onehot
    position = jnp.sum(onehot * before, axis=1)
    keep_mask = position < CAPACITY
    slot_index = jnp.where(keep_mask, expert_idx * CAPACITY + position, buffer_rows)
    source = jax.ops.segment_sum(jnp.arange(ALL_TOKENS, dtype=jnp.int32) + 1, slot_index, num_segments=buffer_rows + 1)[:buffer_rows] - 1
    filled = (source >= 0)[:, None]
    src_safe = jnp.maximum(source, 0)
    slot_safe = jnp.minimum(slot_index, buffer_rows - 1)
    logits = jnp.dot(tokens, w_router, preferred_element_type=jnp.float32)
    router_prob = jax.nn.softmax(logits, axis=-1)
    hot_f = onehot.astype(jnp.float32)
    gate_prob = jnp.sum(hot_f * router_prob, axis=1)
    keep_f = keep_mask.astype(jnp.float32)
    probe_f = loss_probe.astype(jnp.float32)
    g_tok = ((keep_f * gate_prob * grad_scale)[:, None] * probe_f).astype(jnp.bfloat16)
    x_buf = jnp.where(filled, tokens[src_safe], 0).reshape(EXPERTS, CAPACITY, HIDDEN)
    g_buf = jnp.where(filled, g_tok[src_safe], 0).reshape(EXPERTS, CAPACITY, HIDDEN)
    z_buf, u_buf, d_w_in, d_w_out = lax.map(expert_pass, (x_buf, g_buf, w_in, w_out))
    z_tok = jnp.where(keep_mask[:, None], z_buf.reshape(buffer_rows, HIDDEN)[slot_safe], 0).astype(jnp.float32)
    u_tok = jnp.where(keep_mask[:, None], u_buf.reshape(buffer_rows, HIDDEN)[slot_safe], 0).astype(jnp.float32)
    y_out = tokens.astype(jnp.float32) + (keep_f * gate_prob)[:, None] * z_tok
    task_loss = jnp.sum(y_out * probe_f) * grad_scale
    route_frac = jnp.sum(hot_f, axis=0) / ALL_TOKENS
    prob_mean = jnp.mean(router_prob, axis=0)
    loss_value = task_loss + AUX_WEIGHT * EXPERTS * jnp.sum(route_frac * prob_mean)
    d_gate = keep_f * grad_scale * jnp.sum(probe_f * z_tok, axis=1)
    d_logit_task = (d_gate * gate_prob)[:, None] * (hot_f - router_prob)
    aux_coef = AUX_WEIGHT * EXPERTS * route_frac / ALL_TOKENS
    d_logit_aux = router_prob * (aux_coef[None, :] - jnp.sum(router_prob * aux_coef[None, :], axis=1, keepdims=True))
    d_logit = (d_logit_task + d_logit_aux).astype(jnp.bfloat16)
    d_w_router = jnp.dot(tokens.T, d_logit, preferred_element_type=jnp.float32)
    dx_router = jnp.dot(d_logit, w_router.T, preferred_element_type=jnp.float32)
    d_tokens = (grad_scale * probe_f + u_tok + dx_router).astype(jnp.bfloat16)
    return (loss_value, d_tokens, d_w_in, d_w_out, d_w_router)
```

```python
import functools

import jax
import jax.numpy as jnp
from jax import lax
from jax.experimental import pallas as pl
from jax.experimental.pallas import tpu as pltpu
from jax.sharding import PartitionSpec as P

AUX_WEIGHT = 0.01
LANES = 128
MESH = pl.DeviceIdType.MESH
F32 = jnp.float32
BF16 = jnp.bfloat16
ORDER = (8, 4, 2, 12, 10, 6, 14, 9, 5, 3, 13, 11, 7, 15, 1)
VMEM = pl.BlockSpec(memory_space=pltpu.VMEM)
HBM = pl.BlockSpec(memory_space=pl.ANY)
HI = lax.Precision.HIGHEST
NT = (((1,), (1,)), ((), ()))
TN = (((0,), (0,)), ((), ()))


def dot(a, b, dims=(((1,), (0,)), ((), ())), **kw):
    return lax.dot_general(a, b, dims, preferred_element_type=F32, **kw)


def iota(shape, axis):
    return lax.broadcasted_iota(jnp.int32, shape, axis)


def greet(me, groups):
    barrier = pltpu.get_barrier_semaphore()
    for k in range(1, groups):
        pl.semaphore_signal(barrier, inc=1, device_id=(me ^ k,), device_id_type=MESH)
    pl.semaphore_wait(barrier, groups - 1)


def route_kernel(pair_max, idx_ref, x_ref, wr_ref, p_ref, meta_ref, msg_ref):
    experts, tok = p_ref.shape
    idx = idx_ref[...]
    onehot = (iota((experts, tok), 0) == idx).astype(F32)
    upper = (iota((tok, tok), 0) < iota((tok, tok), 1)).astype(BF16)
    before = dot(onehot.astype(BF16), upper)
    rank = jnp.sum(onehot * before, axis=0, keepdims=True)
    logits = dot(wr_ref[...], x_ref[...], NT)
    e = jnp.exp(logits - jnp.max(logits, axis=0, keepdims=True))
    p = e / jnp.sum(e, axis=0, keepdims=True)
    p_ref[...] = p
    gate = jnp.sum(onehot * p, axis=0, keepdims=True)
    rank_hot = (iota((LANES, tok), 0) == rank.astype(jnp.int32)).astype(F32)
    table = dot(onehot * gate, rank_hot, NT, precision=HI)
    count = jnp.sum(onehot, axis=1, keepdims=True)
    lane = iota((experts, LANES), 1)
    row = jnp.where(lane == pair_max, count, jnp.where(lane == pair_max + 1, jnp.sum(p, axis=1, keepdims=True), table))
    msg_ref[...] = row
    meta_ref[0:1, :] = idx * pair_max + rank.astype(jnp.int32)
    meta_ref[1:2, :] = rank.astype(jnp.int32)
    meta_ref[2:, :] = jnp.zeros((meta_ref.shape[0] - 2, tok), jnp.int32)


def pack_kernel(meta_ref, x_ref, r_ref, xs_ref, rs_ref):
    rows, tok = xs_ref.shape[0], x_ref.shape[0]
    base = pl.program_id(0) * rows
    pick = ((iota((rows, tok), 0) + base) == meta_ref[0:1, :]).astype(BF16)
    xs_ref[...] = dot(pick, x_ref[...]).astype(BF16)
    rs_ref[...] = dot(pick, r_ref[...]).astype(BF16)


def expert_kernel(groups, capacity, scale, msg_ref, xs_ref, rs_ref, w1_ref, w2_ref,
                  x_out, h_out, g_out, q_out, u_out, stat_out, rz_out,
                  xbuf, rbuf, mbuf, zsend, zbuf, send, recv, msend, mrecv, zss, zrs, own, xsem):
    e = pl.program_id(0)
    last = pl.num_programs(0) - 1
    me = lax.axis_index('ep')
    pair = xbuf.shape[2]
    hidden = xbuf.shape[3]
    experts = mbuf.shape[1]
    local = xbuf.shape[0]

    def msg_copy(k):
        d = me ^ k
        return pltpu.make_async_remote_copy(
            src_ref=msg_ref, dst_ref=mbuf.at[me], send_sem=msend.at[k], recv_sem=mrecv.at[me],
            device_id=(d,), device_id_type=MESH)

    def msg_got(k):
        d = me ^ k
        return pltpu.make_async_remote_copy(
            src_ref=msg_ref, dst_ref=mbuf.at[d], send_sem=msend.at[k], recv_sem=mrecv.at[d],
            device_id=(d,), device_id_type=MESH)

    def row_copy(t, c, k, src_dev):
        d = me ^ k
        src, buf = ((xs_ref, xbuf), (rs_ref, rbuf))[t]
        return pltpu.make_async_remote_copy(
            src_ref=src.at[d, c], dst_ref=buf.at[c, src_dev], send_sem=send.at[t, c, k],
            recv_sem=recv.at[t, c, src_dev], device_id=(d,), device_id_type=MESH)

    def own_copy(t, c):
        src, buf = ((xs_ref, xbuf), (rs_ref, rbuf))[t]
        return pltpu.make_async_copy(src.at[me, c], buf.at[c, me], own.at[t, c])

    own_msg = pltpu.make_async_copy(msg_ref, mbuf.at[me], mrecv.at[me])

    @pl.when(e == 0)
    def _():
        greet(me, groups)
        own_msg.start()
        for k in ORDER:
            msg_copy(k).start()

        def chunk(c, _):
            for t in range(2):
                own_copy(t, c).start()
                for k in ORDER:
                    row_copy(t, c, k, me).start()
            return 0
        lax.fori_loop(0, local, chunk, 0)
        own_msg.wait()
        for k in ORDER:
            msg_got(k).wait_recv()

    rows = groups * pair
    gates, offs = [], []
    off = jnp.zeros((1, LANES), F32)
    for s in range(groups):
        row = mbuf[s, pl.ds(me * local + e, 1), :]
        gates.append(jnp.broadcast_to(row, (pair, LANES)))
        offs.append(jnp.broadcast_to(off, (pair, LANES)))
        off = off + row
    slot = lax.rem(iota((rows, LANES), 0), pair)
    lane = iota((rows, LANES), 1)
    gate = jnp.sum(jnp.where(lane == slot, jnp.concatenate(gates, axis=0), 0.0), axis=1, keepdims=True)
    ahead = jnp.sum(jnp.where(lane == pair, jnp.concatenate(offs, axis=0), 0.0), axis=1, keepdims=True)
    place = ahead + lax.rem(iota((rows, 1), 0), pair).astype(F32)
    keep = (place < float(capacity)).astype(F32)

    own_copy(0, e).wait()
    for k in ORDER:
        row_copy(0, e, k, me ^ k).wait_recv()
    x_save = pltpu.make_async_copy(xbuf.at[e], x_out.at[e], xsem)
    x_save.start()
    x = xbuf[e].reshape(rows, hidden)
    h = jnp.maximum(dot(x, w1_ref[0]), 0.0).astype(BF16)
    h_out[0] = h
    z = dot(h, w2_ref[0]).astype(BF16).astype(F32)
    own_copy(1, e).wait()
    for k in ORDER:
        row_copy(1, e, k, me ^ k).wait_recv()
    r = rbuf[e].reshape(rows, hidden).astype(F32)
    g = ((keep * gate * scale) * r).astype(BF16)
    g_out[0] = g
    rz = keep * jnp.sum(r * z, axis=1, keepdims=True)
    rz_rows = jnp.sum(jnp.where(lane == slot, rz, 0.0).reshape(groups, pair, LANES), axis=1)
    for s in range(groups):
        zsend[s, pl.ds(e, 1), :] = rz_rows[s:s + 1, :]
    dh = dot(g, w2_ref[0], NT)
    q = jnp.where(h.astype(F32) > 0.0, dh, 0.0).astype(BF16)
    q_out[0] = q
    u_out[...] = dot(q, w1_ref[0], NT).astype(BF16).reshape(groups, 1, pair, hidden)
    x_save.wait()

    @pl.when(e == last)
    def _():
        def z_copy(k, src_dev):
            d = me ^ k
            return pltpu.make_async_remote_copy(
                src_ref=zsend.at[d], dst_ref=zbuf.at[src_dev], send_sem=zss.at[k], recv_sem=zrs.at[src_dev],
                device_id=(d,), device_id_type=MESH)
        mine = pltpu.make_async_copy(zsend.at[me], zbuf.at[me], zrs.at[me])
        mine.start()
        for k in ORDER:
            z_copy(k, me).start()
        for k in ORDER:
            msg_copy(k).wait_send()

        def chunk(c, _):
            for t in range(2):
                for k in ORDER:
                    row_copy(t, c, k, me).wait_send()
            return 0
        lax.fori_loop(0, local, chunk, 0)
        mine.wait()
        for k in ORDER:
            z_copy(k, me ^ k).wait_recv()
        for k in ORDER:
            z_copy(k, me).wait_send()
        stat_out[...] = mbuf[...]
        rz_out[...] = zbuf[...]


def weight_kernel(x_ref, h_ref, g_ref, q_ref, d1_ref, d2_ref):
    d1_ref[0] = dot(x_ref[0], q_ref[0], TN).astype(BF16)
    d2_ref[0] = dot(h_ref[0], g_ref[0], TN).astype(BF16)


def router_kernel(groups, pair, scale, all_tokens, idx_ref, meta_ref, p_ref, stat_ref, rz_ref, x_ref, r_ref,
                  l_out, w_out, loss_out, part, got, red, lsend, lgot, s1, r1, s2, r2, s3, r3):
    me = lax.axis_index('ep')
    greet(me, groups)
    experts, tok = p_ref.shape
    local = experts // groups
    onehot = (iota((experts, tok), 0) == idx_ref[...]).astype(F32)
    rank_hot = iota((LANES, tok), 0) == meta_ref[1:2, :]
    p = p_ref[...]
    gate = jnp.sum(onehot * p, axis=0, keepdims=True)
    table = jnp.concatenate([rz_ref[d, 0:local, :] for d in range(groups)], axis=0)
    rz_all = dot(table, onehot, TN, precision=HI)
    rz = jnp.sum(jnp.where(rank_hot, rz_all, 0.0), axis=0, keepdims=True)
    stat = jnp.zeros((experts, LANES), F32)
    for d in range(groups):
        stat = stat + stat_ref[d]
    lane = iota((experts, LANES), 1)
    total = jnp.sum(jnp.where(lane == pair, stat, 0.0), axis=1, keepdims=True)
    psum = jnp.sum(jnp.where(lane == pair + 1, stat, 0.0), axis=1, keepdims=True)
    frac = total / float(all_tokens)
    aux = AUX_WEIGHT * experts * jnp.sum(frac * (psum / float(all_tokens)), axis=0, keepdims=True)
    coef = (AUX_WEIGHT * experts / all_tokens) * frac
    d_gate = scale * rz
    d_task = (d_gate * gate) * (onehot - p)
    d_aux = p * (coef - jnp.sum(p * coef, axis=0, keepdims=True))
    l = (d_task + d_aux).astype(BF16)
    l_out[...] = l
    for d in range(groups):
        part[d] = dot(l, x_ref[:, d * LANES:(d + 1) * LANES])

    def rs_copy(k, src_dev):
        d = me ^ k
        return pltpu.make_async_remote_copy(
            src_ref=part.at[d], dst_ref=got.at[src_dev], send_sem=s1.at[k], recv_sem=r1.at[src_dev],
            device_id=(d,), device_id_type=MESH)

    def ls_copy(k, src_dev):
        d = me ^ k
        return pltpu.make_async_remote_copy(
            src_ref=lsend, dst_ref=lgot.at[src_dev], send_sem=s3.at[k], recv_sem=r3.at[src_dev],
            device_id=(d,), device_id_type=MESH)

    def ag_copy(k, src_dev):
        d = me ^ k
        return pltpu.make_async_remote_copy(
            src_ref=red, dst_ref=w_out.at[src_dev], send_sem=s2.at[k], recv_sem=r2.at[src_dev],
            device_id=(d,), device_id_type=MESH)

    for k in ORDER:
        rs_copy(k, me).start()
    xr = jnp.sum(jnp.sum(x_ref[...].astype(F32) * r_ref[...].astype(F32), axis=0, keepdims=True), axis=1, keepdims=True)
    mine = xr + jnp.sum(gate * rz, axis=1, keepdims=True)
    lsend[...] = jnp.broadcast_to(mine, lsend.shape)
    for k in ORDER:
        ls_copy(k, me).start()
    for k in ORDER:
        rs_copy(k, me ^ k).wait_recv()
    got[me] = part[me]
    total_w = jnp.zeros(red.shape, F32)
    for d in range(groups):
        total_w = total_w + got[d]
    red[...] = total_w
    for k in ORDER:
        ag_copy(k, me).start()
    for k in ORDER:
        ls_copy(k, me ^ k).wait_recv()
    lgot[me] = lsend[...]
    y = jnp.zeros(lsend.shape, F32)
    for d in range(groups):
        y = y + lgot[d]
    loss_out[...] = y * scale + aux
    w_out[me] = total_w
    for k in ORDER:
        ag_copy(k, me ^ k).wait_recv()
    for k in ORDER:
        rs_copy(k, me).wait_send()
        ls_copy(k, me).wait_send()
        ag_copy(k, me).wait_send()


def token_kernel(scale, meta_ref, u_ref, r_ref, l_ref, wr_ref, o_ref):
    slots, tok = u_ref.shape[0], r_ref.shape[0]
    pick = (iota((slots, tok), 0) == meta_ref[0:1, :]).astype(BF16)
    u = dot(pick, u_ref[...], TN)
    dx = dot(l_ref[...], wr_ref[...], TN)
    o_ref[...] = (scale * r_ref[...].astype(F32) + u + dx).astype(BF16)


def params(**kw):
    return pltpu.CompilerParams(vmem_limit_bytes=62 * 2 ** 20, **kw)


def solution(mesh):
    groups = mesh.shape['ep']

    def local_step(tokens, expert_idx, w_router, w_in, w_out, loss_probe):
        tok, hidden = tokens.shape
        local, _, ffn = w_in.shape
        experts = w_router.shape[1]
        all_tokens = tok * groups
        capacity = (5 * all_tokens + 4 * experts - 1) // (4 * experts)
        pair = 2 * tok // experts
        slots = experts * pair
        rows = groups * pair
        scale = 1.0 / (all_tokens * hidden)
        sds = jax.ShapeDtypeStruct
        idx = expert_idx.reshape(1, tok)
        wr_t = w_router.T

        p_t, meta, msg = pl.pallas_call(
            functools.partial(route_kernel, pair),
            out_shape=[sds((experts, tok), F32), sds((8, tok), jnp.int32), sds((experts, LANES), F32)],
            in_specs=[VMEM] * 3, out_specs=[VMEM] * 3, name='route',
            compiler_params=params())(idx, tokens, wr_t)

        steps = 4
        full = lambda shape: pl.BlockSpec(shape, lambda i: (0,) * len(shape))
        xs, rs = pl.pallas_call(
            pack_kernel, grid=(steps,),
            out_shape=[sds((slots, hidden), BF16)] * 2,
            in_specs=[full((8, tok)), full((tok, hidden)), full((tok, hidden))],
            out_specs=[pl.BlockSpec((slots // steps, hidden), lambda i: (i, 0))] * 2, name='pack',
            compiler_params=params())(meta, tokens, loss_probe)

        per = lambda shape: pl.BlockSpec((1,) + shape, lambda i: (i,) + (0,) * len(shape))
        dma = pltpu.SemaphoreType.DMA
        shape4 = (groups, local, pair, hidden)
        x_buf, h_buf, g_buf, q_buf, u_rows, stat, rz = pl.pallas_call(
            functools.partial(expert_kernel, groups, capacity, scale), grid=(local,),
            out_shape=[sds((local, groups, pair, hidden), BF16), sds((local, rows, ffn), BF16), sds((local, rows, hidden), BF16),
                       sds((local, rows, ffn), BF16), sds(shape4, BF16), sds((groups, experts, LANES), F32), sds((groups, 8, LANES), F32)],
            in_specs=[VMEM, HBM, HBM, per((hidden, ffn)), per((ffn, hidden))],
            out_specs=[HBM, per((rows, ffn)), per((rows, hidden)), per((rows, ffn)),
                       pl.BlockSpec((groups, 1, pair, hidden), lambda i: (0, i, 0, 0)),
                       full((groups, experts, LANES)), full((groups, 8, LANES))],
            scratch_shapes=[pltpu.VMEM((local, groups, pair, hidden), BF16), pltpu.VMEM((local, groups, pair, hidden), BF16),
                            pltpu.VMEM((groups, experts, LANES), F32), pltpu.VMEM((groups, 8, LANES), F32),
                            pltpu.VMEM((groups, 8, LANES), F32), dma((2, local, groups)), dma((2, local, groups)),
                            dma((groups,)), dma((groups,)), dma((groups,)), dma((groups,)), dma((2, local)), dma(())],
            name='experts',
            compiler_params=params(collective_id=0, has_side_effects=True))(
                msg, xs.reshape(shape4), rs.reshape(shape4), w_in, w_out)

        u_back = lax.all_to_all(u_rows, 'ep', 0, 0, tiled=True).reshape(slots, hidden)

        d_w_in, d_w_out = pl.pallas_call(
            weight_kernel, grid=(local,),
            out_shape=[sds((local, hidden, ffn), BF16), sds((local, ffn, hidden), BF16)],
            in_specs=[per((rows, hidden)), per((rows, ffn)), per((rows, hidden)), per((rows, ffn))],
            out_specs=[per((hidden, ffn)), per((ffn, hidden))], name='weights',
            cost_estimate=pl.CostEstimate(flops=4 * local * rows * hidden * ffn, bytes_accessed=50_000_000, transcendentals=0),
            compiler_params=params())(x_buf.reshape(local, rows, hidden), h_buf, g_buf, q_buf)

        l_t, d_wr, loss = pl.pallas_call(
            functools.partial(router_kernel, groups, pair, scale, all_tokens),
            out_shape=[sds((experts, tok), BF16), sds((groups, experts, LANES), F32), sds((8, LANES), F32)],
            in_specs=[VMEM] * 7, out_specs=[VMEM] * 3,
            scratch_shapes=[pltpu.VMEM((groups, experts, LANES), F32), pltpu.VMEM((groups, experts, LANES), F32),
                            pltpu.VMEM((experts, LANES), F32), pltpu.VMEM((8, LANES), F32), pltpu.VMEM((groups, 8, LANES), F32)]
            + [dma((groups,))] * 6, name='router',
            cost_estimate=pl.CostEstimate(flops=30_000_000_000, bytes_accessed=8_000_000, transcendentals=0),
            compiler_params=params(collective_id=1, has_side_effects=True))(
                idx, meta, p_t, stat, rz, tokens, loss_probe)

        cols = hidden // steps
        col = lambda r: pl.BlockSpec((r, cols), lambda i: (0, i))
        d_tokens = pl.pallas_call(
            functools.partial(token_kernel, scale), grid=(steps,),
            out_shape=sds((tok, hidden), BF16),
            in_specs=[full((8, tok)), col(slots), col(tok), full((experts, tok)), col(experts)],
            out_specs=col(tok), name='tokens',
            compiler_params=params())(meta, u_back, loss_probe, l_t, wr_t)

        d_w_router = d_wr.transpose(0, 2, 1).reshape(hidden, experts)
        return loss[0, 0], d_tokens, d_w_in, d_w_out, d_w_router

    in_specs = (P('ep', None), P('ep'), P(None, None), P('ep', None, None), P('ep', None, None), P('ep', None))
    out_specs = (P(), P('ep', None), P('ep', None, None), P('ep', None, None), P(None, None))
    return jax.shard_map(local_step, mesh=mesh, in_specs=in_specs, out_specs=out_specs, check_vma=False)
```

```python
import functools

import jax
import jax.numpy as jnp
from jax import lax
from jax.experimental import pallas as pl
from jax.experimental.pallas import tpu as pltpu
from jax.sharding import PartitionSpec as P

AUX_WEIGHT = 0.01
LANES = 128
MESH = pl.DeviceIdType.MESH
F32 = jnp.float32
BF16 = jnp.bfloat16
ORDER = (8, 4, 2, 12, 10, 6, 14, 9, 5, 3, 13, 11, 7, 15, 1)
VMEM = pl.BlockSpec(memory_space=pltpu.VMEM)
HBM = pl.BlockSpec(memory_space=pl.ANY)
HI = lax.Precision.HIGHEST
NT = (((1,), (1,)), ((), ()))
TN = (((0,), (0,)), ((), ()))


def dot(a, b, dims=(((1,), (0,)), ((), ())), **kw):
    return lax.dot_general(a, b, dims, preferred_element_type=F32, **kw)


def iota(shape, axis):
    return lax.broadcasted_iota(jnp.int32, shape, axis)


def greet(me, groups):
    barrier = pltpu.get_barrier_semaphore()
    for k in range(1, groups):
        pl.semaphore_signal(barrier, inc=1, device_id=(me ^ k,), device_id_type=MESH)
    pl.semaphore_wait(barrier, groups - 1)


def layer_kernel(groups, capacity, scale, all_tokens, idx_ref, x_ref, r_ref, wr_ref, w1_ref, w2_ref,
                 x_out, h_out, g_out, q_out, u_out, u_back, l_out, dwr_out, loss_out, meta_out,
                 xsend, rsend, xbuf, rbuf, usend, msg, mbuf, zsend, zbuf, p_buf, part, got, red, dwr, lsend, lgot,
                 send, recv, msend, mrecv, zss, zrs, uss, urs, s1, r1, s2, r2, s3, r3, own, uown, xsem):
    step = pl.program_id(0)
    last = pl.num_programs(0) - 1
    me = lax.axis_index('ep')
    local, _, pair, hidden = xbuf.shape
    experts, tok = p_buf.shape
    rows = groups * pair
    half = pair // 2
    early = usend.shape[0]

    def remote(src, dst, ssem, rsem, k):
        return pltpu.make_async_remote_copy(src_ref=src, dst_ref=dst, send_sem=ssem, recv_sem=rsem,
                                            device_id=(me ^ k,), device_id_type=MESH)

    def msg_copy(k, dev):
        return remote(msg, mbuf.at[dev], msend.at[k], mrecv.at[dev], k)

    def row_copy(t, c, k, dev):
        src, buf = ((xsend, xbuf), (rsend, rbuf))[t]
        return remote(src.at[c, me ^ k], buf.at[c, dev], send.at[t, c, k], recv.at[t, c, dev], k)

    def own_copy(t, c):
        src, buf = ((xsend, xbuf), (rsend, rbuf))[t]
        return pltpu.make_async_copy(src.at[c, me], buf.at[c, me], own.at[t, c])

    def z_copy(k, dev):
        return remote(zsend.at[me ^ k], zbuf.at[dev], zss.at[k], zrs.at[dev], k)

    def u_copy(c, s, k, dev):
        return remote(usend.at[c, me ^ k, pl.ds(s * half, half)], u_back.at[dev, c, pl.ds(s * half, half)],
                      uss.at[c, s, k], urs.at[c, s, dev], k)

    def u_own(c):
        return pltpu.make_async_copy(usend.at[c, me], u_back.at[me, c], uown.at[c])

    def rs_copy(k, dev):
        return remote(part.at[me ^ k], got.at[dev], s1.at[k], r1.at[dev], k)

    def ls_copy(k, dev):
        return remote(lsend, lgot.at[dev], s3.at[k], r3.at[dev], k)

    def ag_copy(k, dev):
        return remote(red, dwr.at[dev], s2.at[k], r2.at[dev], k)

    @pl.when(step == 0)
    def _():
        greet(me, groups)
        idx = idx_ref[...]
        onehot = (iota((experts, tok), 0) == idx).astype(F32)
        upper = (iota((tok, tok), 0) < iota((tok, tok), 1)).astype(BF16)
        before = dot(onehot.astype(BF16), upper)
        rank = jnp.sum(onehot * before, axis=0, keepdims=True).astype(jnp.int32)
        slot_of = idx * pair + rank
        meta_out[0:1, :] = slot_of
        meta_out[1:2, :] = rank
        meta_out[2:, :] = jnp.zeros((meta_out.shape[0] - 2, tok), jnp.int32)

        def chunk(c, _):
            row = iota((rows, tok), 0)
            want = (row // pair) * (local * pair) + c * pair + lax.rem(row, pair)
            pick = (want == slot_of).astype(BF16)
            xsend[c] = dot(pick, x_ref[...]).astype(BF16).reshape(groups, pair, hidden)
            rsend[c] = dot(pick, r_ref[...]).astype(BF16).reshape(groups, pair, hidden)
            for t in range(2):
                own_copy(t, c).start()
                for k in ORDER:
                    row_copy(t, c, k, me).start()
            return 0

        chunk(0, 0)
        logits = dot(wr_ref[...], x_ref[...], NT)
        ex = jnp.exp(logits - jnp.max(logits, axis=0, keepdims=True))
        p = ex / jnp.sum(ex, axis=0, keepdims=True)
        p_buf[...] = p
        gate = jnp.sum(onehot * p, axis=0, keepdims=True)
        rank_hot = (iota((LANES, tok), 0) == rank).astype(F32)
        table = dot(onehot * gate, rank_hot, NT, precision=HI)
        lane = iota((experts, LANES), 1)
        msg[...] = jnp.where(lane == pair, jnp.sum(onehot, axis=1, keepdims=True),
                             jnp.where(lane == pair + 1, jnp.sum(p, axis=1, keepdims=True), table))
        for k in ORDER:
            msg_copy(k, me).start()
        lax.fori_loop(1, local, chunk, 0)
        mbuf[me] = msg[...]
        for k in ORDER:
            msg_copy(k, me ^ k).wait_recv()

    @pl.when(step == 1)
    def _():
        prod = x_ref[...].astype(F32) * r_ref[...].astype(F32)
        xr = jnp.sum(jnp.sum(prod, axis=0, keepdims=True), axis=1, keepdims=True)
        lsend[...] = jnp.broadcast_to(xr, lsend.shape)

    gates, offs = [], []
    off = jnp.zeros((1, LANES), F32)
    for s in range(groups):
        row = mbuf[s, pl.ds(me * local + step, 1), :]
        gates.append(jnp.broadcast_to(row, (pair, LANES)))
        offs.append(jnp.broadcast_to(off, (pair, LANES)))
        off = off + row
    slot = lax.rem(iota((rows, LANES), 0), pair)
    lane = iota((rows, LANES), 1)
    gate = jnp.sum(jnp.where(lane == slot, jnp.concatenate(gates, axis=0), 0.0), axis=1, keepdims=True)
    ahead = jnp.sum(jnp.where(lane == pair, jnp.concatenate(offs, axis=0), 0.0), axis=1, keepdims=True)
    place = ahead + lax.rem(iota((rows, 1), 0), pair).astype(F32)
    keep = (place < float(capacity)).astype(F32)

    own_copy(0, step).wait()
    for k in ORDER:
        row_copy(0, step, k, me ^ k).wait_recv()
    x_save = pltpu.make_async_copy(xbuf.at[step], x_out.at[step], xsem)
    x_save.start()
    h = jnp.maximum(dot(xbuf[step].reshape(rows, hidden), w1_ref[0]), 0.0).astype(BF16)
    h_out[0] = h
    z = dot(h, w2_ref[0]).astype(BF16).astype(F32)
    own_copy(1, step).wait()
    for k in ORDER:
        row_copy(1, step, k, me ^ k).wait_recv()
    r = rbuf[step].reshape(rows, hidden).astype(F32)
    rz = keep * jnp.sum(r * z, axis=1, keepdims=True)
    rz_rows = jnp.sum(jnp.where(lane == slot, rz, 0.0).reshape(groups, pair, LANES), axis=1)
    for s in range(groups):
        zsend[s, pl.ds(step, 1), :] = rz_rows[s:s + 1, :]
    g = ((keep * gate * scale) * r).astype(BF16)
    g_out[0] = g

    @pl.when(step == last)
    def _():
        for k in ORDER:
            z_copy(k, me).start()
        for k in ORDER:
            u_copy(0, 0, k, me).start()

    dh = dot(g, w2_ref[0], NT)
    q = jnp.where(h_out[0].astype(F32) > 0.0, dh, 0.0).astype(BF16)
    q_out[0] = q
    u = dot(q, w1_ref[0], NT).astype(BF16)

    @pl.when(step < early)
    def _():
        usend[step] = u.reshape(groups, pair, hidden)

    @pl.when(step >= early)
    def _():
        u_out[...] = u.reshape(groups, 1, pair, hidden)

    x_save.wait()

    @pl.when(step == last)
    def _():
        zbuf[me] = zsend[me]
        for k in ORDER:
            z_copy(k, me ^ k).wait_recv()
        onehot = (iota((experts, tok), 0) == idx_ref[...]).astype(F32)
        rank_hot = iota((LANES, tok), 0) == meta_out[1:2, :]
        p = p_buf[...]
        gate = jnp.sum(onehot * p, axis=0, keepdims=True)
        table = jnp.concatenate([zbuf[d, 0:local, :] for d in range(groups)], axis=0)
        rz_all = dot(table, onehot, TN, precision=HI)
        rz = jnp.sum(jnp.where(rank_hot, rz_all, 0.0), axis=0, keepdims=True)
        stat = jnp.zeros((experts, LANES), F32)
        for d in range(groups):
            stat = stat + mbuf[d]
        lane = iota((experts, LANES), 1)
        frac = jnp.sum(jnp.where(lane == pair, stat, 0.0), axis=1, keepdims=True) / float(all_tokens)
        p_mean = jnp.sum(jnp.where(lane == pair + 1, stat, 0.0), axis=1, keepdims=True) / float(all_tokens)
        aux = AUX_WEIGHT * experts * jnp.sum(frac * p_mean, axis=0, keepdims=True)
        coef = (AUX_WEIGHT * experts / all_tokens) * frac
        d_task = ((scale * rz) * gate) * (onehot - p)
        d_aux = p * (coef - jnp.sum(p * coef, axis=0, keepdims=True))
        l = (d_task + d_aux).astype(BF16)
        l_out[...] = l
        for d in range(groups):
            part[d] = dot(l, x_ref[:, d * LANES:(d + 1) * LANES])
        lsend[...] = lsend[...] + jnp.sum(gate * rz, axis=1, keepdims=True)
        for k in ORDER:
            rs_copy(k, me).start()
        for k in ORDER:
            ls_copy(k, me).start()
        for k in ORDER:
            u_copy(0, 1, k, me).start()
        for c in range(early):
            u_own(c).start()
        for k in ORDER:
            rs_copy(k, me ^ k).wait_recv()
        got[me] = part[me]
        total = got[0]
        for d in range(1, groups):
            total = total + got[d]
        red[...] = total
        for k in ORDER:
            ag_copy(k, me).start()
        for c in range(1, early):
            for s in range(2):
                for k in ORDER:
                    u_copy(c, s, k, me).start()
        for k in ORDER:
            ls_copy(k, me ^ k).wait_recv()
        lgot[me] = lsend[...]
        y = lgot[0]
        for d in range(1, groups):
            y = y + lgot[d]
        loss_out[...] = y * scale + aux
        dwr[me] = total
        for k in ORDER:
            ag_copy(k, me ^ k).wait_recv()
        dwr_out[...] = dwr[...]
        for c in range(early):
            for s in range(2):
                for k in ORDER:
                    u_copy(c, s, k, me ^ k).wait_recv()
            u_own(c).wait()
        for k in ORDER:
            msg_copy(k, me).wait_send()
            z_copy(k, me).wait_send()
            rs_copy(k, me).wait_send()
            ls_copy(k, me).wait_send()
            ag_copy(k, me).wait_send()

        def sent(c, _):
            for t in range(2):
                for k in ORDER:
                    row_copy(t, c, k, me).wait_send()
            return 0
        lax.fori_loop(0, local, sent, 0)
        for c in range(early):
            for s in range(2):
                for k in ORDER:
                    u_copy(c, s, k, me).wait_send()


def weight_kernel(x_ref, h_ref, g_ref, q_ref, d1_ref, d2_ref):
    d1_ref[0] = dot(x_ref[0], q_ref[0], TN).astype(BF16)
    d2_ref[0] = dot(h_ref[0], g_ref[0], TN).astype(BF16)


def picked(meta_ref, first, pair, early, local, count, tok):
    row = iota((count, tok), 0)
    span = early * pair
    want = (row // span) * (local * pair) + first * pair + lax.rem(row, span)
    return (want == meta_ref[0:1, :]).astype(BF16)


def token_first_kernel(scale, pair, early, local, meta_ref, u_ref, r_ref, l_ref, wr_ref, o_ref):
    pick = picked(meta_ref, 0, pair, early, local, u_ref.shape[0], r_ref.shape[0])
    u = dot(pick, u_ref[...], TN)
    dx = dot(l_ref[...], wr_ref[...], TN)
    o_ref[...] = scale * r_ref[...].astype(F32) + u + dx


def token_last_kernel(pair, early, local, meta_ref, u_ref, a_ref, o_ref):
    pick = picked(meta_ref, early, pair, local - early, local, u_ref.shape[0], a_ref.shape[0])
    o_ref[...] = (a_ref[...] + dot(pick, u_ref[...], TN)).astype(BF16)


def params(**kw):
    return pltpu.CompilerParams(vmem_limit_bytes=62 * 2 ** 20, **kw)


def solution(mesh):
    groups = mesh.shape['ep']

    def local_step(tokens, expert_idx, w_router, w_in, w_out, loss_probe):
        tok, hidden = tokens.shape
        local, _, ffn = w_in.shape
        experts = w_router.shape[1]
        all_tokens = tok * groups
        capacity = (5 * all_tokens + 4 * experts - 1) // (4 * experts)
        pair = 2 * tok // experts
        slots = experts * pair
        rows = groups * pair
        scale = 1.0 / (all_tokens * hidden)
        sds = jax.ShapeDtypeStruct
        idx = expert_idx.reshape(1, tok)
        wr_t = w_router.T

        steps = 4
        early = 2
        full = lambda shape: pl.BlockSpec(shape, lambda i: (0,) * len(shape))
        per = lambda shape: pl.BlockSpec((1,) + shape, lambda i: (i,) + (0,) * len(shape))
        vm = lambda *shape: pltpu.VMEM(shape, BF16)
        vf = lambda *shape: pltpu.VMEM(shape, F32)
        dma = lambda *shape: pltpu.SemaphoreType.DMA(shape)
        x_buf, h_buf, g_buf, q_buf, u_late, u_early, l_t, d_wr, loss, meta = pl.pallas_call(
            functools.partial(layer_kernel, groups, capacity, scale, all_tokens), grid=(local,),
            out_shape=[sds((local, groups, pair, hidden), BF16), sds((local, rows, ffn), BF16), sds((local, rows, hidden), BF16),
                       sds((local, rows, ffn), BF16), sds((groups, local - early, pair, hidden), BF16),
                       sds((groups, early, pair, hidden), BF16), sds((experts, tok), BF16),
                       sds((groups, experts, LANES), F32), sds((8, LANES), F32), sds((8, tok), jnp.int32)],
            in_specs=[VMEM, VMEM, VMEM, VMEM, per((hidden, ffn)), per((ffn, hidden))],
            out_specs=[HBM, per((rows, ffn)), per((rows, hidden)), per((rows, ffn)),
                       pl.BlockSpec((groups, 1, pair, hidden), lambda i: (0, jnp.maximum(i - early, 0), 0, 0)),
                       HBM, VMEM, VMEM, VMEM, VMEM],
            scratch_shapes=[vm(local, groups, pair, hidden)] * 4
            + [vm(early, groups, pair, hidden), vf(experts, LANES), vf(groups, experts, LANES), vf(groups, 8, LANES),
               vf(groups, 8, LANES), vf(experts, tok), vf(groups, experts, LANES), vf(groups, experts, LANES),
               vf(experts, LANES), vf(groups, experts, LANES), vf(8, LANES), vf(groups, 8, LANES),
               dma(2, local, groups), dma(2, local, groups)] + [dma(groups)] * 4
            + [dma(early, 2, groups)] * 2 + [dma(groups)] * 6 + [dma(2, local), dma(early), pltpu.SemaphoreType.DMA],
            name='layer',
            compiler_params=params(collective_id=0, has_side_effects=True))(
                idx, tokens, loss_probe, wr_t, w_in, w_out)

        u_late = lax.all_to_all(u_late, 'ep', 0, 0, tiled=True).reshape(groups * (local - early) * pair, hidden)
        u_early = u_early.reshape(groups * early * pair, hidden)

        d_w_in, d_w_out = pl.pallas_call(
            weight_kernel, grid=(local,),
            out_shape=[sds((local, hidden, ffn), BF16), sds((local, ffn, hidden), BF16)],
            in_specs=[per((rows, hidden)), per((rows, ffn)), per((rows, hidden)), per((rows, ffn))],
            out_specs=[per((hidden, ffn)), per((ffn, hidden))], name='weights',
            cost_estimate=pl.CostEstimate(flops=4 * local * rows * hidden * ffn, bytes_accessed=50_000_000, transcendentals=0),
            compiler_params=params())(x_buf.reshape(local, rows, hidden), h_buf, g_buf, q_buf)

        cols = hidden // steps
        col = lambda r: pl.BlockSpec((r, cols), lambda i: (0, i))
        acc = pl.pallas_call(
            functools.partial(token_first_kernel, scale, pair, early, local), grid=(steps,),
            out_shape=sds((tok, hidden), F32),
            in_specs=[full((8, tok)), col(u_early.shape[0]), col(tok), full((experts, tok)), col(experts)],
            out_specs=col(tok), name='first',
            cost_estimate=pl.CostEstimate(flops=4_000_000_000, bytes_accessed=8_000_000, transcendentals=0),
            compiler_params=params())(meta, u_early, loss_probe, l_t, wr_t)
        d_tokens = pl.pallas_call(
            functools.partial(token_last_kernel, pair, early, local), grid=(steps,),
            out_shape=sds((tok, hidden), BF16),
            in_specs=[full((8, tok)), col(u_late.shape[0]), col(tok)],
            out_specs=col(tok), name='last',
            compiler_params=params())(meta, u_late, acc)

        d_w_router = d_wr.transpose(0, 2, 1).reshape(hidden, experts)
        return loss[0, 0], d_tokens, d_w_in, d_w_out, d_w_router

    in_specs = (P('ep', None), P('ep'), P(None, None), P('ep', None, None), P('ep', None, None), P('ep', None))
    out_specs = (P(), P('ep', None), P('ep', None, None), P('ep', None, None), P(None, None))
    return jax.shard_map(local_step, mesh=mesh, in_specs=in_specs, out_specs=out_specs, check_vma=False)
```

```python
import functools

import jax
import jax.numpy as jnp
from jax import lax
from jax.experimental import pallas as pl
from jax.experimental.pallas import tpu as pltpu
from jax.sharding import PartitionSpec as P

AUX_WEIGHT = 0.01
LANES = 128
MESH = pl.DeviceIdType.MESH
F32 = jnp.float32
BF16 = jnp.bfloat16
ORDER = (8, 4, 2, 12, 10, 6, 14, 9, 5, 3, 13, 11, 7, 15, 1)
VMEM = pl.BlockSpec(memory_space=pltpu.VMEM)
HBM = pl.BlockSpec(memory_space=pl.ANY)
HI = lax.Precision.HIGHEST
NT = (((1,), (1,)), ((), ()))
TN = (((0,), (0,)), ((), ()))


def dot(a, b, dims=(((1,), (0,)), ((), ())), **kw):
    return lax.dot_general(a, b, dims, preferred_element_type=F32, **kw)


def iota(shape, axis):
    return lax.broadcasted_iota(jnp.int32, shape, axis)


def greet(me, groups):
    barrier = pltpu.get_barrier_semaphore()
    for k in range(1, groups):
        pl.semaphore_signal(barrier, inc=1, device_id=(me ^ k,), device_id_type=MESH)
    pl.semaphore_wait(barrier, groups - 1)


def layer_kernel(groups, capacity, scale, all_tokens, idx_ref, x_ref, r_ref, wr_ref, w1_hbm, w2_hbm,
                 x_out, h_out, g_out, q_out, u_out, u_back, l_out, dwr_out, loss_out, meta_out,
                 xsend, rsend, xbuf, rbuf, usend, msg, mbuf, zsend, zbuf, p_buf, part, sib, got, red, dwr, lsend, lgot, w1_buf, w2_buf,
                 send, recv, msend, mrecv, zss, zrs, uss, urs, s1, r1, s2, r2, s3, r3, cs, own, uown, xsem, wsem):
    step = pl.program_id(0)
    last = pl.num_programs(0) - 1
    me = lax.axis_index('ep')
    local, _, pair, hidden = xbuf.shape
    experts, tok = p_buf.shape
    rows = groups * pair
    half = pair // 2
    early = usend.shape[0]
    chips = groups // 2
    chip, core = me // 2, lax.rem(me, 2)
    far = tuple(k for k in ORDER if k % 2 == 0)

    def remote(src, dst, ssem, rsem, k):
        return pltpu.make_async_remote_copy(src_ref=src, dst_ref=dst, send_sem=ssem, recv_sem=rsem,
                                            device_id=(me ^ k,), device_id_type=MESH)

    def msg_copy(k, dev):
        return remote(msg.at[me ^ k], mbuf.at[dev], msend.at[k], mrecv.at[dev], k)

    def row_copy(t, c, k, dev):
        src, buf = ((xsend, xbuf), (rsend, rbuf))[t]
        return remote(src.at[c, me ^ k], buf.at[c, dev], send.at[t, c, k], recv.at[t, c, dev], k)

    def own_copy(t, c):
        src, buf = ((xsend, xbuf), (rsend, rbuf))[t]
        return pltpu.make_async_copy(src.at[c, me], buf.at[c, me], own.at[t, c])

    def z_copy(k, dev):
        return remote(zsend.at[me ^ k], zbuf.at[dev], zss.at[k], zrs.at[dev], k)

    def u_copy(c, s, k, dev):
        return remote(usend.at[c, me ^ k, pl.ds(s * half, half)], u_back.at[dev, c, pl.ds(s * half, half)],
                      uss.at[c, s, k], urs.at[c, s, dev], k)

    def u_own(c):
        return pltpu.make_async_copy(usend.at[c, me], u_back.at[me, c], uown.at[c])

    def pair_copy():
        return remote(part.at[1 - core], sib, cs.at[0], cs.at[1], 1)

    def rs_copy(k, dev):
        return remote(part.at[core, (me ^ k) // 2], got.at[dev // 2], s1.at[k], r1.at[dev // 2], k)

    def ls_copy(k, dev):
        return remote(lsend, lgot.at[dev], s3.at[k], r3.at[dev], k)

    def ag_copy(k, dev):
        return remote(red, dwr.at[core, dev // 2], s2.at[k], r2.at[dev // 2], k)

    def share_copy(b):
        return remote(dwr.at[b], dwr.at[b], cs.at[2], cs.at[3], 1)

    def w_copy(t, e):
        src, buf = ((w1_hbm, w1_buf), (w2_hbm, w2_buf))[t]
        return pltpu.make_async_copy(src.at[e], buf.at[lax.rem(e, 2)], wsem.at[t, lax.rem(e, 2)])

    @pl.when(step == 0)
    def _():
        greet(me, groups)
        idx = idx_ref[...]
        onehot = (iota((experts, tok), 0) == idx).astype(F32)
        upper = (iota((tok, tok), 0) < iota((tok, tok), 1)).astype(BF16)
        before = dot(onehot.astype(BF16), upper)
        rank = jnp.sum(onehot * before, axis=0, keepdims=True).astype(jnp.int32)
        slot_of = idx * pair + rank
        meta_out[0:1, :] = slot_of
        meta_out[1:2, :] = rank
        meta_out[2:, :] = jnp.zeros((meta_out.shape[0] - 2, tok), jnp.int32)

        def chunk(c, _):
            row = iota((rows, tok), 0)
            want = (row // pair) * (local * pair) + c * pair + lax.rem(row, pair)
            pick = (want == slot_of).astype(BF16)
            xsend[c] = dot(pick, x_ref[...]).astype(BF16).reshape(groups, pair, hidden)
            rsend[c] = dot(pick, r_ref[...]).astype(BF16).reshape(groups, pair, hidden)
            for t in range(2):
                own_copy(t, c).start()
                for k in ORDER:
                    row_copy(t, c, k, me).start()
            return 0

        chunk(0, 0)
        for t in range(2):
            w_copy(t, 0).start()
        logits = dot(wr_ref[...], x_ref[...], NT)
        ex = jnp.exp(logits - jnp.max(logits, axis=0, keepdims=True))
        p = ex / jnp.sum(ex, axis=0, keepdims=True)
        p_buf[...] = p
        gate = jnp.sum(onehot * p, axis=0, keepdims=True)
        rank_hot = (iota((LANES, tok), 0) == rank).astype(F32)
        table = dot(onehot * gate, rank_hot, NT, precision=HI)
        lane = iota((experts, LANES), 1)
        ones = jnp.ones((8, tok), F32)
        counts = dot(ones.astype(BF16), onehot.astype(BF16), NT)
        p_sums = dot(ones, p, NT, precision=HI)
        table = jnp.where(lane == pair, jnp.sum(onehot, axis=1, keepdims=True), table)
        for d in range(groups):
            msg[d, 0:local, :] = table[d * local:(d + 1) * local, :]
            msg[d, local:local + 1, 0:experts] = counts[0:1, :]
            msg[d, local + 1:local + 2, 0:experts] = p_sums[0:1, :]
            msg[d, local:local + 2, experts:] = jnp.zeros((2, LANES - experts), F32)
            msg[d, local + 2:, :] = jnp.zeros((msg.shape[1] - local - 2, LANES), F32)
        for k in ORDER:
            msg_copy(k, me).start()
        lax.fori_loop(1, local, chunk, 0)
        mbuf[me] = msg[me]
        for k in ORDER:
            msg_copy(k, me ^ k).wait_recv()

    @pl.when(step == 1)
    def _():
        prod = x_ref[...].astype(F32) * r_ref[...].astype(F32)
        xr = jnp.sum(jnp.sum(prod, axis=0, keepdims=True), axis=1, keepdims=True)
        lsend[...] = jnp.broadcast_to(xr, lsend.shape)

    gates, offs = [], []
    off = jnp.zeros((1, LANES), F32)
    for s in range(groups):
        row = mbuf[s, pl.ds(step, 1), :]
        gates.append(jnp.broadcast_to(row, (pair, LANES)))
        offs.append(jnp.broadcast_to(off, (pair, LANES)))
        off = off + row
    slot = lax.rem(iota((rows, LANES), 0), pair)
    lane = iota((rows, LANES), 1)
    gate = jnp.sum(jnp.where(lane == slot, jnp.concatenate(gates, axis=0), 0.0), axis=1, keepdims=True)
    ahead = jnp.sum(jnp.where(lane == pair, jnp.concatenate(offs, axis=0), 0.0), axis=1, keepdims=True)
    place = ahead + lax.rem(iota((rows, 1), 0), pair).astype(F32)
    keep = (place < float(capacity)).astype(F32)

    for t in range(2):
        w_copy(t, step).wait()

    @pl.when(step < last)
    def _():
        for t in range(2):
            w_copy(t, step + 1).start()

    slot_w = lax.rem(step, 2)
    own_copy(0, step).wait()
    for k in ORDER:
        row_copy(0, step, k, me ^ k).wait_recv()
    x_save = pltpu.make_async_copy(xbuf.at[step], x_out.at[step], xsem)
    x_save.start()
    h = jnp.maximum(dot(xbuf[step].reshape(rows, hidden), w1_buf[slot_w]), 0.0).astype(BF16)
    h_out[0] = h
    z = dot(h, w2_buf[slot_w]).astype(BF16).astype(F32)
    own_copy(1, step).wait()
    for k in ORDER:
        row_copy(1, step, k, me ^ k).wait_recv()
    r = rbuf[step].reshape(rows, hidden).astype(F32)
    rz = keep * jnp.sum(r * z, axis=1, keepdims=True)
    rz_rows = jnp.sum(jnp.where(lane == slot, rz, 0.0).reshape(groups, pair, LANES), axis=1)
    for s in range(groups):
        zsend[s, pl.ds(step, 1), :] = rz_rows[s:s + 1, :]
    g = ((keep * gate * scale) * r).astype(BF16)
    g_out[0] = g

    @pl.when(step == last)
    def _():
        for k in ORDER:
            z_copy(k, me).start()
        for k in ORDER:
            u_copy(0, 0, k, me).start()

    dh = dot(g, w2_buf[slot_w], NT)
    q = jnp.where(h_out[0].astype(F32) > 0.0, dh, 0.0).astype(BF16)
    q_out[0] = q
    u = dot(q, w1_buf[slot_w], NT).astype(BF16)

    @pl.when(step < early)
    def _():
        usend[step] = u.reshape(groups, pair, hidden)

    @pl.when(step >= early)
    def _():
        u_out[...] = u.reshape(groups, 1, pair, hidden)

    x_save.wait()

    @pl.when(step == last)
    def _():
        zbuf[me] = zsend[me]
        for k in ORDER:
            z_copy(k, me ^ k).wait_recv()
        onehot = (iota((experts, tok), 0) == idx_ref[...]).astype(F32)
        rank_hot = iota((LANES, tok), 0) == meta_out[1:2, :]
        p = p_buf[...]
        gate = jnp.sum(onehot * p, axis=0, keepdims=True)
        table = jnp.concatenate([zbuf[d, 0:local, :] for d in range(groups)], axis=0)
        rz_all = dot(table, onehot, TN, precision=HI)
        rz = jnp.sum(jnp.where(rank_hot, rz_all, 0.0), axis=0, keepdims=True)
        stat = mbuf[0]
        for d in range(1, groups):
            stat = stat + mbuf[d]
        diag = iota((experts, LANES), 0) == iota((experts, LANES), 1)
        frac = jnp.sum(jnp.where(diag, stat[local:local + 1, :], 0.0), axis=1, keepdims=True) / float(all_tokens)
        p_mean = jnp.sum(jnp.where(diag, stat[local + 1:local + 2, :], 0.0), axis=1, keepdims=True) / float(all_tokens)
        aux = AUX_WEIGHT * experts * jnp.sum(frac * p_mean, axis=0, keepdims=True)
        coef = (AUX_WEIGHT * experts / all_tokens) * frac
        d_task = ((scale * rz) * gate) * (onehot - p)
        d_aux = p * (coef - jnp.sum(p * coef, axis=0, keepdims=True))
        l = (d_task + d_aux).astype(BF16)
        l_out[...] = l
        for d in range(chips):
            both = dot(l, x_ref[:, 2 * d * LANES:2 * (d + 1) * LANES])
            part[0, d] = both[:, :LANES]
            part[1, d] = both[:, LANES:]
        lsend[...] = lsend[...] + jnp.sum(gate * rz, axis=1, keepdims=True)
        pair_copy().start()
        for k in ORDER:
            ls_copy(k, me).start()
        for k in ORDER:
            u_copy(0, 1, k, me).start()
        for c in range(early):
            u_own(c).start()
        pair_copy().wait_recv()
        for d in range(chips):
            part[core, d] = part[core, d] + sib[d]
        for k in far:
            rs_copy(k, me).start()
        for k in ORDER:
            u_copy(1, 0, k, me).start()
        for k in far:
            rs_copy(k, me ^ k).wait_recv()
        got[chip] = part[core, chip]
        total = got[0]
        for d in range(1, chips):
            total = total + got[d]
        red[...] = total
        for k in far:
            ag_copy(k, me).start()
        for k in ORDER:
            u_copy(1, 1, k, me).start()
        for k in ORDER:
            ls_copy(k, me ^ k).wait_recv()
        lgot[me] = lsend[...]
        y = lgot[0]
        for d in range(1, groups):
            y = y + lgot[d]
        loss_out[...] = y * scale + aux
        dwr[core, chip] = total
        for k in far:
            ag_copy(k, me ^ k).wait_recv()
        share_copy(core).start()
        share_copy(1 - core).wait_recv()
        for d in range(groups):
            dwr_out[:, d * LANES:(d + 1) * LANES] = dwr[d % 2, d // 2]
        for c in range(early):
            for s in range(2):
                for k in ORDER:
                    u_copy(c, s, k, me ^ k).wait_recv()
            u_own(c).wait()
        for k in ORDER:
            msg_copy(k, me).wait_send()
            z_copy(k, me).wait_send()
            ls_copy(k, me).wait_send()
        for k in far:
            rs_copy(k, me).wait_send()
            ag_copy(k, me).wait_send()
        pair_copy().wait_send()
        share_copy(core).wait_send()

        def sent(c, _):
            for t in range(2):
                for k in ORDER:
                    row_copy(t, c, k, me).wait_send()
            return 0
        lax.fori_loop(0, local, sent, 0)
        for c in range(early):
            for s in range(2):
                for k in ORDER:
                    u_copy(c, s, k, me).wait_send()


def weight_kernel(x_ref, h_ref, g_ref, q_ref, d1_ref, d2_ref):
    d1_ref[0] = dot(x_ref[0], q_ref[0], TN).astype(BF16)
    d2_ref[0] = dot(h_ref[0], g_ref[0], TN).astype(BF16)


def pick_kernel(pair, early, local, meta_ref, first_ref, rest_ref):
    tok = meta_ref.shape[1]
    row = meta_ref[0:1, :].astype(F32)
    slot = jnp.sum(jnp.where(iota((tok, tok), 0) == iota((tok, tok), 1), row, 0.0), axis=1, keepdims=True).astype(jnp.int32)
    for first, count, o_ref in ((0, early, first_ref), (early, local - early, rest_ref)):
        col = iota(o_ref.shape, 1)
        span = count * pair
        want = (col // span) * (local * pair) + first * pair + lax.rem(col, span)
        o_ref[...] = (want == slot).astype(BF16)


def token_kernel(scale, pick1_ref, pick2_ref, u1_ref, u2_ref, r_ref, l_ref, wr_ref, o_ref):
    u = dot(pick1_ref[...], u1_ref[...]) + dot(pick2_ref[...], u2_ref[...])
    dx = dot(l_ref[...], wr_ref[...], TN)
    o_ref[...] = (scale * r_ref[...].astype(F32) + u + dx).astype(BF16)


def params(**kw):
    return pltpu.CompilerParams(vmem_limit_bytes=62 * 2 ** 20, **kw)


def solution(mesh):
    groups = mesh.shape['ep']

    def local_step(tokens, expert_idx, w_router, w_in, w_out, loss_probe):
        tok, hidden = tokens.shape
        local, _, ffn = w_in.shape
        experts = w_router.shape[1]
        all_tokens = tok * groups
        capacity = (5 * all_tokens + 4 * experts - 1) // (4 * experts)
        pair = 2 * tok // experts
        slots = experts * pair
        rows = groups * pair
        scale = 1.0 / (all_tokens * hidden)
        sds = jax.ShapeDtypeStruct
        idx = expert_idx.reshape(1, tok)
        wr_t = w_router.T

        steps = 4
        early = 2
        full = lambda shape: pl.BlockSpec(shape, lambda i: (0,) * len(shape))
        per = lambda shape: pl.BlockSpec((1,) + shape, lambda i: (i,) + (0,) * len(shape))
        vm = lambda *shape: pltpu.VMEM(shape, BF16)
        vf = lambda *shape: pltpu.VMEM(shape, F32)
        dma = lambda *shape: pltpu.SemaphoreType.DMA(shape)
        x_buf, h_buf, g_buf, q_buf, u_late, u_early, l_t, d_wr, loss, meta = pl.pallas_call(
            functools.partial(layer_kernel, groups, capacity, scale, all_tokens), grid=(local,),
            out_shape=[sds((local, groups, pair, hidden), BF16), sds((local, rows, ffn), BF16), sds((local, rows, hidden), BF16),
                       sds((local, rows, ffn), BF16), sds((groups, local - early, pair, hidden), BF16),
                       sds((groups, early, pair, hidden), BF16), sds((experts, tok), BF16),
                       sds((experts, hidden), F32), sds((8, LANES), F32), sds((8, tok), jnp.int32)],
            in_specs=[VMEM, VMEM, VMEM, VMEM, HBM, HBM],
            out_specs=[HBM, per((rows, ffn)), per((rows, hidden)), per((rows, ffn)),
                       pl.BlockSpec((groups, 1, pair, hidden), lambda i: (0, jnp.maximum(i - early, 0), 0, 0)),
                       HBM, VMEM, VMEM, VMEM, VMEM],
            scratch_shapes=[vm(local, groups, pair, hidden)] * 4
            + [vm(early, groups, pair, hidden)] + [vf(groups, 8, LANES)] * 4
            + [vf(experts, tok), vf(2, groups // 2, experts, LANES), vf(groups // 2, experts, LANES), vf(groups // 2, experts, LANES),
               vf(experts, LANES), vf(2, groups // 2, experts, LANES), vf(8, LANES), vf(groups, 8, LANES),
               vm(2, hidden, ffn), vm(2, ffn, hidden), dma(2, local, groups), dma(2, local, groups)] + [dma(groups)] * 4
            + [dma(early, 2, groups)] * 2 + [dma(groups)] * 6
            + [dma(4), dma(2, local), dma(early), pltpu.SemaphoreType.DMA, dma(2, 2)],
            name='layer',
            compiler_params=params(collective_id=0, has_side_effects=True))(
                idx, tokens, loss_probe, wr_t, w_in, w_out)

        u_late = lax.all_to_all(u_late, 'ep', 0, 0, tiled=True).reshape(groups * (local - early) * pair, hidden)
        u_early = u_early.reshape(groups * early * pair, hidden)

        d_w_in, d_w_out = pl.pallas_call(
            weight_kernel, grid=(local,),
            out_shape=[sds((local, hidden, ffn), BF16), sds((local, ffn, hidden), BF16)],
            in_specs=[per((rows, hidden)), per((rows, ffn)), per((rows, hidden)), per((rows, ffn))],
            out_specs=[per((hidden, ffn)), per((ffn, hidden))], name='weights',
            cost_estimate=pl.CostEstimate(flops=4 * local * rows * hidden * ffn, bytes_accessed=50_000_000, transcendentals=0),
            compiler_params=params())(x_buf.reshape(local, rows, hidden), h_buf, g_buf, q_buf)

        cols = hidden // steps
        col = lambda r: pl.BlockSpec((r, cols), lambda i: (0, i))
        pick1, pick2 = pl.pallas_call(
            functools.partial(pick_kernel, pair, early, local),
            out_shape=[sds((tok, u_early.shape[0]), BF16), sds((tok, u_late.shape[0]), BF16)],
            in_specs=[VMEM], out_specs=[VMEM] * 2, name='pick',
            cost_estimate=pl.CostEstimate(flops=2_000_000_000, bytes_accessed=1_000_000, transcendentals=0),
            compiler_params=params())(meta)
        d_tokens = pl.pallas_call(
            functools.partial(token_kernel, scale), grid=(steps,),
            out_shape=sds((tok, hidden), BF16),
            in_specs=[full(pick1.shape), full(pick2.shape), col(u_early.shape[0]), col(u_late.shape[0]), col(tok),
                      full((experts, tok)), col(experts)],
            out_specs=col(tok), name='tokens',
            compiler_params=params())(pick1, pick2, u_early, u_late, loss_probe, l_t, wr_t)

        d_w_router = d_wr.T
        return loss[0, 0], d_tokens, d_w_in, d_w_out, d_w_router

    in_specs = (P('ep', None), P('ep'), P(None, None), P('ep', None, None), P('ep', None, None), P('ep', None))
    out_specs = (P(), P('ep', None), P('ep', None, None), P('ep', None, None), P(None, None))
    return jax.shard_map(local_step, mesh=mesh, in_specs=in_specs, out_specs=out_specs, check_vma=False)
```
